32 devices in a mesh: py: 4 (over x, core), px: 8 (over z, y).
Axes of the slice: x: 2, y: 2, z: 4, core: 2. Of those that a mesh axis runs over, the one named last changes fastest.
Arguments:
- source_terms: float32 [256, 1024, 256], P('py', 'px'), may hold values from -6 to 6
- initial_values: float32 [256, 1024, 256], P('py', 'px'), may hold values from -6 to 6
- absorption: float32 [256, 1024, 256], P('py', 'px'), may hold values from 0.1 to 0.9
Outputs:
- solution: float32 [256, 1024, 256], P('py', 'px')
- remaining: float32 [256, 1024, 256], P('py', 'px')
The draws below stay inside these ranges and needn't reach their ends.
All inputs are finite; a program needn't handle non-finite values.
Results may differ from the reference program's by a relative error of at most 0.000033.
Values sent between devices are 32-bit elements; how exact they have to be, the bound alone decides.
A program may use at most 128 MiB of HBM per device.

```python
import jax
import jax.numpy as jnp
from jax import lax

LAYERS = 256
RATIO = 2
BEFORE = 2
AFTER = 2
INNER = 9
GRID_Y = 256
GRID_X = 1024


def shard_levels(stream_key, shape, split, smallest, top_value):
    def one(axis_at, blocks):
        steps = jax.random.uniform(jax.random.fold_in(jax.random.fold_in(stream_key, 6), axis_at), (blocks,), jnp.float32, smallest / len(split), top_value / len(split))
        return jnp.repeat(jnp.exp(steps), shape[axis_at] // blocks).reshape((-1,) + (1,) * (len(shape) - axis_at - 1))

    level = one(*split[0])
    for cut in split[1:]:
        level = level * one(*cut)
    return level


def gaussian(stream_key, extent, deviation, bound, shards=(), kind=jnp.bfloat16):
    array = jax.random.normal(stream_key, extent, jnp.float32) * deviation
    if len(shards) > 0:
        array = shard_levels(stream_key, extent, shards, -0.22, 0.18) * array
    return jnp.clip(array, min=-bound, max=bound).astype(kind)


def setup_inputs(seed: int = 0) -> dict:
    key_of = jax.random.split(jax.random.key(seed), 4)
    source_terms = gaussian(key_of[0], (GRID_Y, GRID_X, LAYERS), 1.0, 6.0, ((0, 4), (1, 8)), jnp.float32)
    initial_values = gaussian(key_of[1], (GRID_Y, GRID_X, LAYERS), 1.0, 6.0, ((0, 4), (1, 8)), jnp.float32)
    absorption = jnp.clip(0.1 + 0.79999997 * jax.random.uniform(key_of[2], (GRID_Y, GRID_X, LAYERS), jnp.float32) ** shard_levels(key_of[2], (GRID_Y, GRID_X, LAYERS), ((0, 4), (1, 8)), -0.2, 0.2), 0.1, 0.9)
    return dict(source_terms=source_terms, initial_values=initial_values, absorption=absorption)


def around_sum(padded):
    inner_y, inner_x = padded.shape[0] - 2, padded.shape[1] - 2
    middle_rows = lax.slice_in_dim(padded, 1, 1 + inner_y, axis=0)
    middle_columns = lax.slice_in_dim(padded, 1, 1 + inner_x, axis=1)
    return (lax.slice_in_dim(middle_columns, 0, inner_y, axis=0) + lax.slice_in_dim(middle_columns, 2, 2 + inner_y, axis=0)
            + lax.slice_in_dim(middle_rows, 0, inner_x, axis=1) + lax.slice_in_dim(middle_rows, 2, 2 + inner_x, axis=1))


def relax_once(padded, values, load, mass_here):
    return values + 0.8 * (load + around_sum(padded) - (4.0 + mass_here) * values) / (4.0 + mass_here)


def block_means(values):
    cut = values.reshape(values.shape[0] // RATIO, RATIO, values.shape[1] // RATIO, RATIO, values.shape[2])
    return jnp.mean(cut, axis=(1, 3))


def spread_blocks(values):
    return jnp.repeat(jnp.repeat(values, RATIO, axis=0), RATIO, axis=1)


def reference(source_terms, initial_values, absorption):
    values = initial_values
    for sweep in range(BEFORE):
        values = relax_once(jnp.pad(values, ((1, 1), (1, 1), (0, 0)), mode="wrap"), values, source_terms, absorption)
    defect = source_terms + around_sum(jnp.pad(values, ((1, 1), (1, 1), (0, 0)), mode="wrap")) - (4.0 + absorption) * values
    coarse_load, coarse_mass = block_means(defect) * RATIO, block_means(absorption) * RATIO
    coarse_values = jnp.zeros_like(coarse_load)
    for sweep in range(INNER):
        coarse_values = relax_once(jnp.pad(coarse_values, ((1, 1), (1, 1), (0, 0)), mode="wrap"), coarse_values, coarse_load, coarse_mass)
    values = values + spread_blocks(coarse_values)
    for sweep in range(AFTER):
        values = relax_once(jnp.pad(values, ((1, 1), (1, 1), (0, 0)), mode="wrap"), values, source_terms, absorption)
    solution = values
    remaining = source_terms + around_sum(jnp.pad(solution, ((1, 1), (1, 1), (0, 0)), mode="wrap")) - (4.0 + absorption) * solution
    return solution, remaining
```

```python
import functools

import jax
import jax.numpy as jnp
from jax import lax
from jax.experimental import pallas as pl
from jax.experimental.pallas import tpu as pltpu
from jax.sharding import PartitionSpec as P

INNER = 9
LANES = 128
PAD = 8
MESH = pl.DeviceIdType.MESH


def kernel(
    sizes, load_in, start_in, mass_in, solution_out, remaining_out,
    one, two, load, mass, rate, coarse_one, coarse_two, coarse_load, coarse_rate,
    pair, side_send, side_recv, in_sem, out_sem, send_sem, recv_sem,
):
    chunks, ny, nx, count_y, count_x = sizes
    cy, cx = ny // 2, nx // 2
    my_y, my_x = lax.axis_index("py"), lax.axis_index("px")
    targets = (
        {"py": lax.rem(my_y + count_y - 1, count_y)},
        {"py": lax.rem(my_y + 1, count_y)},
        {"px": lax.rem(my_x + count_x - 1, count_x)},
        {"px": lax.rem(my_x + 1, count_x)},
    )

    def fetch(c, kind):
        part = pl.ds(c * LANES, LANES)
        if kind == 0:
            source, target = start_in, one.at[c, pl.ds(1, ny), pl.ds(PAD, nx), :]
        elif kind == 1:
            source, target = mass_in, mass.at[c]
        else:
            source, target = load_in, load.at[c]
        return pltpu.make_async_copy(source.at[:, :, part], target, in_sem.at[c, kind])

    def put(c, kind):
        source, target = ((one, solution_out), (two, remaining_out))[kind]
        return pltpu.make_async_copy(
            source.at[c, pl.ds(1, ny), pl.ds(PAD, nx), :],
            target.at[:, :, pl.ds(c * LANES, LANES)],
            out_sem.at[c, kind],
        )

    def copies(cells, c, turn, rows, columns):
        ends = (
            (cells.at[c, 1, pl.ds(PAD, columns), :], cells.at[c, rows + 1, pl.ds(PAD, columns), :]),
            (cells.at[c, rows, pl.ds(PAD, columns), :], cells.at[c, 0, pl.ds(PAD, columns), :]),
            (side_send.at[turn, c, 0, pl.ds(0, rows), :], side_recv.at[turn, c, 1, pl.ds(0, rows), :]),
            (side_send.at[turn, c, 1, pl.ds(0, rows), :], side_recv.at[turn, c, 0, pl.ds(0, rows), :]),
        )
        return [
            pltpu.make_async_remote_copy(
                src_ref=source,
                dst_ref=target,
                send_sem=send_sem.at[turn, c, way],
                recv_sem=recv_sem.at[turn, c, way],
                device_id=targets[way],
                device_id_type=MESH,
            )
            for way, (source, target) in enumerate(ends)
        ]

    def send(*where):
        for copy in copies(*where):
            copy.start()

    def receive(cells, c, turn, rows, columns):
        for copy in copies(cells, c, turn, rows, columns):
            copy.wait()

        def place(y, carry):
            cells[c, y + 1, pl.ds(PAD - 1, 1), :] = side_recv[turn, c, 0, pl.ds(y, 1), :]
            cells[c, y + 1, pl.ds(PAD + columns, 1), :] = side_recv[turn, c, 1, pl.ds(y, 1), :]
            return carry

        lax.fori_loop(0, rows, place, 0, unroll=8)

    def blocks(columns):
        size = min(columns, 64)
        return [(at, size) for at in range(0, columns, size)]

    def around(cells, c, y, at, size):
        return (
            (cells[c, y, pl.ds(PAD + at, size), :] + cells[c, y + 2, pl.ds(PAD + at, size), :])
            + cells[c, y + 1, pl.ds(PAD + at - 1, size), :]
        ) + cells[c, y + 1, pl.ds(PAD + at + 1, size), :]

    def keep(source, target, c, turn, y, at, size, columns, new):
        target[c, y + 1, pl.ds(PAD + at, size), :] = new
        if at == 0:
            side_send[turn, c, 0, pl.ds(y, 1), :] = new[0:1, :]
        if at + size == columns:
            side_send[turn, c, 1, pl.ds(y, 1), :] = new[size - 1 : size, :]

    def fine_sweep(source, target, c, turn, first):
        def row(y, carry):
            for at, size in blocks(nx):
                if first:
                    speed = 0.8 / (4.0 + mass[c, y, pl.ds(at, size), :])
                    rate[c, y, pl.ds(at, size), :] = speed
                else:
                    speed = rate[c, y, pl.ds(at, size), :]
                total = load[c, y, pl.ds(at, size), :] + around(source, c, y, at, size)
                new = 0.2 * source[c, y + 1, pl.ds(PAD + at, size), :] + speed * total
                keep(source, target, c, turn, y, at, size, nx, new)
            return carry

        lax.fori_loop(0, ny, row, 0)

    def coarse_sweep(source, target, c, turn):
        def row(y, carry):
            for at, size in blocks(cx):
                total = coarse_load[c, y, pl.ds(at, size), :] + around(source, c, y, at, size)
                new = (
                    0.2 * source[c, y + 1, pl.ds(PAD + at, size), :]
                    + coarse_rate[c, y, pl.ds(at, size), :] * total
                )
                keep(source, target, c, turn, y, at, size, cx, new)
            return carry

        lax.fori_loop(0, cy, row, 0)

    def defect(cells, c, y, at, size):
        return (load[c, y, pl.ds(at, size), :] + around(cells, c, y, at, size)) - (
            4.0 + mass[c, y, pl.ds(at, size), :]
        ) * cells[c, y + 1, pl.ds(PAD + at, size), :]

    def restrict(cells, c, turn):
        def row(y, carry):
            for at, size in blocks(nx):
                pair[0, pl.ds(at, size), :] = defect(cells, c, 2 * y, at, size) + defect(
                    cells, c, 2 * y + 1, at, size
                )
                pair[1, pl.ds(at, size), :] = (
                    mass[c, 2 * y, pl.ds(at, size), :] + mass[c, 2 * y + 1, pl.ds(at, size), :]
                )
            here = 0.5 * (pair[0, pl.ds(0, cx, stride=2), :] + pair[0, pl.ds(1, cx, stride=2), :])
            zero_order = 0.5 * (
                pair[1, pl.ds(0, cx, stride=2), :] + pair[1, pl.ds(1, cx, stride=2), :]
            )
            speed = 0.8 / (4.0 + zero_order)
            coarse_load[c, y] = here
            coarse_rate[c, y] = speed
            keep(None, coarse_one, c, turn, y, 0, cx, cx, speed * here)
            return carry

        lax.fori_loop(0, cy, row, 0)

    def correct_row(c, fine_row, coarse_row):
        extra = coarse_one[c, coarse_row, pl.ds(PAD, cx), :]
        for shift in range(2):
            spot = pl.ds(PAD + shift, cx, stride=2)
            one[c, fine_row, spot, :] = one[c, fine_row, spot, :] + extra

    def correct(c):
        correct_row(c, 0, 0)
        correct_row(c, ny + 1, cy + 1)

        def row(y, carry):
            for half in range(2):
                fine_row = 2 * y + 1 + half
                correct_row(c, fine_row, y + 1)
                for here, there in ((PAD - 1, PAD - 1), (PAD + nx, PAD + cx)):
                    one[c, fine_row, pl.ds(here, 1), :] = (
                        one[c, fine_row, pl.ds(here, 1), :]
                        + coarse_one[c, y + 1, pl.ds(there, 1), :]
                    )
            return carry

        lax.fori_loop(0, cy, row, 0)

    every = range(chunks)
    for c in every:
        for kind in range(3):
            fetch(c, kind).start()

    barrier = pltpu.get_barrier_semaphore()
    for target in targets:
        pl.semaphore_signal(barrier, inc=1, device_id=target, device_id_type=MESH)
    pl.semaphore_wait(barrier, 4)

    for c in every:
        fetch(c, 0).wait()

        def sides(y, carry):
            side_send[0, c, 0, pl.ds(y, 1), :] = one[c, y + 1, pl.ds(PAD, 1), :]
            side_send[0, c, 1, pl.ds(y, 1), :] = one[c, y + 1, pl.ds(PAD + nx - 1, 1), :]
            return carry

        lax.fori_loop(0, ny, sides, 0, unroll=8)
        send(one, c, 0, ny, nx)
    for c in every:
        fetch(c, 1).wait()
        fetch(c, 2).wait()
        receive(one, c, 0, ny, nx)
        fine_sweep(one, two, c, 1, True)
        send(two, c, 1, ny, nx)
    for c in every:
        receive(two, c, 1, ny, nx)
        fine_sweep(two, one, c, 0, False)
        send(one, c, 0, ny, nx)
    for c in every:
        receive(one, c, 0, ny, nx)
        restrict(one, c, 1)
        send(coarse_one, c, 1, cy, cx)

    def couple(step, carry):
        for c in every:
            receive(coarse_one, c, 1, cy, cx)
            coarse_sweep(coarse_one, coarse_two, c, 0)
            send(coarse_two, c, 0, cy, cx)
        for c in every:
            receive(coarse_two, c, 0, cy, cx)
            coarse_sweep(coarse_two, coarse_one, c, 1)
            send(coarse_one, c, 1, cy, cx)
        return carry

    lax.fori_loop(0, (INNER - 1) // 2, couple, 0)
    for c in every:
        receive(coarse_one, c, 1, cy, cx)
        correct(c)
        fine_sweep(one, two, c, 0, False)
        send(two, c, 0, ny, nx)
    for c in every:
        receive(two, c, 0, ny, nx)
        fine_sweep(two, one, c, 1, False)
        send(one, c, 1, ny, nx)
        put(c, 0).start()

    for c in every:
        receive(one, c, 1, ny, nx)

        def row(y, carry):
            for at, size in blocks(nx):
                two[c, y + 1, pl.ds(PAD + at, size), :] = defect(one, c, y, at, size)
            return carry

        lax.fori_loop(0, ny, row, 0)
        put(c, 1).start()
    for c in every:
        for kind in range(2):
            put(c, kind).wait()


def local(count_y, count_x, source_terms, initial_values, absorption):
    ny, nx, layers = source_terms.shape
    chunks = layers // LANES
    cy, cx = ny // 2, nx // 2
    kind = jnp.float32
    fine = pltpu.VMEM((chunks, ny, nx, LANES), kind)
    wide = pltpu.VMEM((chunks, ny + 2, nx + 2 * PAD, LANES), kind)
    coarse = pltpu.VMEM((chunks, cy, cx, LANES), kind)
    coarse_wide = pltpu.VMEM((chunks, cy + 2, cx + 2 * PAD, LANES), kind)
    side = pltpu.VMEM((2, chunks, 2, ny, LANES), kind)
    out = jax.ShapeDtypeStruct(source_terms.shape, kind)
    return pl.pallas_call(
        functools.partial(kernel, (chunks, ny, nx, count_y, count_x)),
        out_shape=(out, out),
        in_specs=[pl.BlockSpec(memory_space=pl.ANY)] * 3,
        out_specs=[pl.BlockSpec(memory_space=pl.ANY)] * 2,
        scratch_shapes=[
            wide, wide, fine, fine, fine, coarse_wide, coarse_wide, coarse, coarse,
            pltpu.VMEM((2, nx, LANES), kind), side, side,
            pltpu.SemaphoreType.DMA((chunks, 3)),
            pltpu.SemaphoreType.DMA((chunks, 2)),
            pltpu.SemaphoreType.DMA((2, chunks, 4)),
            pltpu.SemaphoreType.DMA((2, chunks, 4)),
        ],
        compiler_params=pltpu.CompilerParams(
            collective_id=0, has_side_effects=True, vmem_limit_bytes=66_000_000
        ),
    )(source_terms, initial_values, absorption)


def solution(mesh):
    spec = P("py", "px", None)
    return jax.shard_map(
        functools.partial(local, mesh.shape["py"], mesh.shape["px"]),
        mesh=mesh,
        in_specs=(spec, spec, spec),
        out_specs=(spec, spec),
        check_vma=False,
    )
```

```python
import functools

import jax
import jax.numpy as jnp
from jax import lax
from jax.experimental import pallas as pl
from jax.experimental.pallas import tpu as pltpu
from jax.sharding import PartitionSpec as P

INNER = 9
LANES = 128
PAD = 8
MESH = pl.DeviceIdType.MESH


def kernel(
    sizes, load_in, start_in, mass_in, solution_out, remaining_out,
    one, two, load, mass, rate, coarse_one, coarse_two, coarse_load, coarse_rate,
    pair, side_send, side_recv, in_sem, out_sem, send_sem, recv_sem,
):
    chunks, ny, nx, count_y, count_x = sizes
    cy, cx = ny // 2, nx // 2
    my_y, my_x = lax.axis_index("py"), lax.axis_index("px")
    targets = (
        {"py": lax.rem(my_y + count_y - 1, count_y)},
        {"py": lax.rem(my_y + 1, count_y)},
        {"px": lax.rem(my_x + count_x - 1, count_x)},
        {"px": lax.rem(my_x + 1, count_x)},
    )

    def fetch(c, kind):
        part = pl.ds(c * LANES, LANES)
        if kind == 0:
            source, target = start_in, one.at[c, pl.ds(1, ny), pl.ds(PAD, nx), :]
        elif kind == 1:
            source, target = mass_in, mass.at[c]
        else:
            source, target = load_in, load.at[c]
        return pltpu.make_async_copy(source.at[:, :, part], target, in_sem.at[c, kind])

    def put(c, kind):
        source, target = ((one, solution_out), (two, remaining_out))[kind]
        return pltpu.make_async_copy(
            source.at[c, pl.ds(1, ny), pl.ds(PAD, nx), :],
            target.at[:, :, pl.ds(c * LANES, LANES)],
            out_sem.at[c, kind],
        )

    def copies(cells, c, turn, rows, columns):
        ends = (
            (cells.at[c, 1, pl.ds(PAD, columns), :], cells.at[c, rows + 1, pl.ds(PAD, columns), :]),
            (cells.at[c, rows, pl.ds(PAD, columns), :], cells.at[c, 0, pl.ds(PAD, columns), :]),
            (side_send.at[turn, c, 0, pl.ds(0, rows), :], side_recv.at[turn, c, 1, pl.ds(0, rows), :]),
            (side_send.at[turn, c, 1, pl.ds(0, rows), :], side_recv.at[turn, c, 0, pl.ds(0, rows), :]),
        )
        return [
            pltpu.make_async_remote_copy(
                src_ref=source,
                dst_ref=target,
                send_sem=send_sem.at[turn, c, way],
                recv_sem=recv_sem.at[turn, c, way],
                device_id=targets[way],
                device_id_type=MESH,
            )
            for way, (source, target) in enumerate(ends)
        ]

    def send(*where):
        for copy in copies(*where):
            copy.start()

    def receive(cells, c, turn, rows, columns):
        for copy in copies(cells, c, turn, rows, columns):
            copy.wait()

        def place(y, carry):
            cells[c, y + 1, pl.ds(PAD - 1, 1), :] = side_recv[turn, c, 0, pl.ds(y, 1), :]
            cells[c, y + 1, pl.ds(PAD + columns, 1), :] = side_recv[turn, c, 1, pl.ds(y, 1), :]
            return carry

        lax.fori_loop(0, rows, place, 0, unroll=8)

    def blocks(columns):
        size = min(columns, 64)
        return [(at, size) for at in range(0, columns, size)]

    def around(cells, c, y, at, size):
        return (
            (cells[c, y, pl.ds(PAD + at, size), :] + cells[c, y + 2, pl.ds(PAD + at, size), :])
            + cells[c, y + 1, pl.ds(PAD + at - 1, size), :]
        ) + cells[c, y + 1, pl.ds(PAD + at + 1, size), :]

    def keep(target, c, y, at, size, new):
        target[c, y + 1, pl.ds(PAD + at, size), :] = new

    def sweep(target, c, turn, rows, columns, value):
        def row(y, carry):
            for at, size in blocks(columns):
                keep(target, c, y, at, size, value(y, at, size))
            return carry

        def sides(y, carry):
            side_send[turn, c, 0, pl.ds(y, 1), :] = value(y, 0, PAD)[0:1, :]
            side_send[turn, c, 1, pl.ds(y, 1), :] = value(y, columns - PAD, PAD)[PAD - 1 : PAD, :]
            return carry

        row(0, 0)
        row(rows - 1, 0)
        lax.fori_loop(0, rows, sides, 0, unroll=8)
        send(target, c, turn, rows, columns)
        lax.fori_loop(1, rows - 1, row, 0, unroll=2)

    def fine_sweep(source, target, c, turn, first):
        def value(y, at, size):
            if first:
                speed = 0.8 / (4.0 + mass[c, y, pl.ds(at, size), :])
                rate[c, y, pl.ds(at, size), :] = speed
            else:
                speed = rate[c, y, pl.ds(at, size), :]
            total = load[c, y, pl.ds(at, size), :] + around(source, c, y, at, size)
            return 0.2 * source[c, y + 1, pl.ds(PAD + at, size), :] + speed * total

        sweep(target, c, turn, ny, nx, value)

    def coarse_sweep(source, target, c, turn):
        def value(y, at, size):
            total = coarse_load[c, y, pl.ds(at, size), :] + around(source, c, y, at, size)
            return (
                0.2 * source[c, y + 1, pl.ds(PAD + at, size), :]
                + coarse_rate[c, y, pl.ds(at, size), :] * total
            )

        sweep(target, c, turn, cy, cx, value)

    def defect(cells, c, y, at, size):
        return (load[c, y, pl.ds(at, size), :] + around(cells, c, y, at, size)) - (
            4.0 + mass[c, y, pl.ds(at, size), :]
        ) * cells[c, y + 1, pl.ds(PAD + at, size), :]

    def restrict(cells, c, turn):
        def row(y, carry):
            for at, size in blocks(nx):
                pair[0, pl.ds(at, size), :] = defect(cells, c, 2 * y, at, size) + defect(
                    cells, c, 2 * y + 1, at, size
                )
                pair[1, pl.ds(at, size), :] = (
                    mass[c, 2 * y, pl.ds(at, size), :] + mass[c, 2 * y + 1, pl.ds(at, size), :]
                )
            here = 0.5 * (pair[0, pl.ds(0, cx, stride=2), :] + pair[0, pl.ds(1, cx, stride=2), :])
            zero_order = 0.5 * (
                pair[1, pl.ds(0, cx, stride=2), :] + pair[1, pl.ds(1, cx, stride=2), :]
            )
            speed = 0.8 / (4.0 + zero_order)
            coarse_load[c, y] = here
            coarse_rate[c, y] = speed
            new = speed * here
            keep(coarse_one, c, y, 0, cx, new)
            side_send[turn, c, 0, pl.ds(y, 1), :] = new[0:1, :]
            side_send[turn, c, 1, pl.ds(y, 1), :] = new[cx - 1 : cx, :]
            return carry

        lax.fori_loop(0, cy, row, 0, unroll=4)

    def correct_row(c, fine_row, coarse_row):
        extra = coarse_one[c, coarse_row, pl.ds(PAD, cx), :]
        for shift in range(2):
            spot = pl.ds(PAD + shift, cx, stride=2)
            one[c, fine_row, spot, :] = one[c, fine_row, spot, :] + extra

    def correct(c):
        correct_row(c, 0, 0)
        correct_row(c, ny + 1, cy + 1)

        def row(y, carry):
            for half in range(2):
                fine_row = 2 * y + 1 + half
                correct_row(c, fine_row, y + 1)
                for here, there in ((PAD - 1, PAD - 1), (PAD + nx, PAD + cx)):
                    one[c, fine_row, pl.ds(here, 1), :] = (
                        one[c, fine_row, pl.ds(here, 1), :]
                        + coarse_one[c, y + 1, pl.ds(there, 1), :]
                    )
            return carry

        lax.fori_loop(0, cy, row, 0, unroll=4)

    every = range(chunks)
    for c in every:
        for kind in range(3):
            fetch(c, kind).start()

    barrier = pltpu.get_barrier_semaphore()
    for target in targets:
        pl.semaphore_signal(barrier, inc=1, device_id=target, device_id_type=MESH)
    pl.semaphore_wait(barrier, 4)

    for c in every:
        fetch(c, 0).wait()

        def sides(y, carry):
            side_send[0, c, 0, pl.ds(y, 1), :] = one[c, y + 1, pl.ds(PAD, 1), :]
            side_send[0, c, 1, pl.ds(y, 1), :] = one[c, y + 1, pl.ds(PAD + nx - 1, 1), :]
            return carry

        lax.fori_loop(0, ny, sides, 0, unroll=8)
        send(one, c, 0, ny, nx)
    for c in every:
        fetch(c, 1).wait()
        fetch(c, 2).wait()
        receive(one, c, 0, ny, nx)
        fine_sweep(one, two, c, 1, True)
    for c in every:
        receive(two, c, 1, ny, nx)
        fine_sweep(two, one, c, 0, False)
    for c in every:
        receive(one, c, 0, ny, nx)
        restrict(one, c, 1)
        send(coarse_one, c, 1, cy, cx)

    def couple(step, carry):
        for c in every:
            receive(coarse_one, c, 1, cy, cx)
            coarse_sweep(coarse_one, coarse_two, c, 0)
        for c in every:
            receive(coarse_two, c, 0, cy, cx)
            coarse_sweep(coarse_two, coarse_one, c, 1)
        return carry

    lax.fori_loop(0, (INNER - 1) // 2, couple, 0)
    for c in every:
        receive(coarse_one, c, 1, cy, cx)
        correct(c)
        fine_sweep(one, two, c, 0, False)
    for c in every:
        receive(two, c, 0, ny, nx)
        fine_sweep(two, one, c, 1, False)
        put(c, 0).start()

    for c in every:
        receive(one, c, 1, ny, nx)

        def row(y, carry):
            for at, size in blocks(nx):
                two[c, y + 1, pl.ds(PAD + at, size), :] = defect(one, c, y, at, size)
            return carry

        lax.fori_loop(0, ny, row, 0, unroll=4)
        put(c, 1).start()
    for c in every:
        for kind in range(2):
            put(c, kind).wait()


def local(count_y, count_x, source_terms, initial_values, absorption):
    ny, nx, layers = source_terms.shape
    chunks = layers // LANES
    cy, cx = ny // 2, nx // 2
    kind = jnp.float32
    fine = pltpu.VMEM((chunks, ny, nx, LANES), kind)
    wide = pltpu.VMEM((chunks, ny + 2, nx + 2 * PAD, LANES), kind)
    coarse = pltpu.VMEM((chunks, cy, cx, LANES), kind)
    coarse_wide = pltpu.VMEM((chunks, cy + 2, cx + 2 * PAD, LANES), kind)
    side = pltpu.VMEM((2, chunks, 2, ny, LANES), kind)
    out = jax.ShapeDtypeStruct(source_terms.shape, kind)
    return pl.pallas_call(
        functools.partial(kernel, (chunks, ny, nx, count_y, count_x)),
        out_shape=(out, out),
        in_specs=[pl.BlockSpec(memory_space=pl.ANY)] * 3,
        out_specs=[pl.BlockSpec(memory_space=pl.ANY)] * 2,
        scratch_shapes=[
            wide, wide, fine, fine, fine, coarse_wide, coarse_wide, coarse, coarse,
            pltpu.VMEM((2, nx, LANES), kind), side, side,
            pltpu.SemaphoreType.DMA((chunks, 3)),
            pltpu.SemaphoreType.DMA((chunks, 2)),
            pltpu.SemaphoreType.DMA((2, chunks, 4)),
            pltpu.SemaphoreType.DMA((2, chunks, 4)),
        ],
        compiler_params=pltpu.CompilerParams(
            collective_id=0, has_side_effects=True, vmem_limit_bytes=66_000_000
        ),
    )(source_terms, initial_values, absorption)


def solution(mesh):
    spec = P("py", "px", None)
    return jax.shard_map(
        functools.partial(local, mesh.shape["py"], mesh.shape["px"]),
        mesh=mesh,
        in_specs=(spec, spec, spec),
        out_specs=(spec, spec),
        check_vma=False,
    )
```
